32 devices in a mesh: grp: 32 (over z, y, x, core), fft: 1.
Axes of the slice: x: 2, y: 2, z: 4, core: 2. Of those that a mesh axis runs over, the one named last changes fastest.
Arguments:
- noise: bfloat16 [1920, 2, 256, 256], P('grp', None, 'fft'), may hold values from -6 to 6
- root: bfloat16 [1920, 256, 256], P('grp', 'fft'), may hold values from 0.25 to 2
- home: int32 [1920, 1], replicated, may hold values from 0 to 31; in each aligned block of 60 rows (0 to 59, 60 to 119, ...) at most 2 rows name the same one
Outputs:
- sample: bfloat16 [32, 32, 2, 256, 256], P('grp', None, None, 'fft')
The draws below stay inside these ranges and needn't reach their ends.
Inputs may be any that keep to these rules, and one draw needn't show every extreme that they name: Among the 60 fields of one source group (aligned blocks of 60 entries), at most 2 have the same home group.
All inputs are finite; a program needn't handle non-finite values.
Results may differ from the reference program's by a relative error of at most 0.0066.
Values may be sent and summed in bfloat16 or wider, within the bound.
No kernel may reach another device: no remote copies, remote signals or barrier semaphores. Data moves between devices by JAX's collectives and lax.ppermute only.
A program may use at most 192 MiB of HBM per device.

```python
import math
import jax
import jax.numpy as jnp
import numpy as np
from jax import lax

L = 256
FSRC = 60
CAP = 2
FIELDS = 1920
N_GRP = 32


def shard_levels(own_key, dims, shards, low, largest):
    factor_of = 1.0
    for axis_at, shards_of in shards:
        draws = jax.random.uniform(jax.random.fold_in(jax.random.fold_in(own_key, 6), axis_at), (shards_of,), jnp.float32, low / len(shards), largest / len(shards))
        factor_of = factor_of * jnp.repeat(jnp.exp(draws), dims[axis_at] // shards_of).reshape((-1,) + (1,) * (len(dims) - 1 - axis_at))
    return factor_of


def shared_out(key, own, number, rows, number_of, top, bound, slope):
    ranking = jax.random.permutation(key, number_of)
    heavy_load, usual = load_shares(number_of, rows * top, bound, slope, True), load_shares(number_of, rows * top, bound, slope, False)
    places = jnp.arange(number_of)

    def named(lengths, rotation):
        used = int((lengths > 0).sum())
        fixed = max(1, used // 4)
        passed = fixed + (places - fixed + rotation * (used - fixed)) % max(1, number_of - fixed)
        return jnp.zeros((number_of,), jnp.int32).at[ranking[jnp.where(places < fixed, places, passed)]].set(jnp.asarray(lengths, jnp.int32))

    lengths = jnp.where(number % 4 == 0, named(heavy_load, number // 4), named(usual, number - number // 4 - 1))
    mixed = jax.random.permutation(jax.random.fold_in(own, 3), number_of)
    donor, sink = mixed[0:number_of // 2 * 2:2], mixed[1:number_of // 2 * 2:2]
    slack = jnp.minimum(lengths[donor] - 1, bound - lengths[sink]) // 2
    slack = jnp.where((donor == ranking[0]) | (sink == ranking[0]) | (lengths[sink] == 0), 0, jnp.maximum(slack, 0))
    passed = jax.random.randint(jax.random.fold_in(own, 4), (number_of // 2,), 0, 1 << 20) % (slack + 1)
    lengths = lengths.at[donor].add(-passed).at[sink].add(passed)
    items = jnp.searchsorted(jnp.cumsum(lengths), jnp.arange(rows * top), side="right").astype(jnp.int32)
    table = items.reshape(top, rows).T
    table = table[jax.random.permutation(jax.random.fold_in(own, 1), rows)]
    rotation = jax.random.randint(jax.random.fold_in(own, 2), (rows, 1), 0, top)
    return jnp.take_along_axis(table, (jnp.arange(top)[None, :] + rotation) % top, axis=1)


def load_shares(number_of, total, most, slope, full):
    weights = [(1 << 20) // math.isqrt(standing ** slope) + 1 for standing in range(1, number_of + 1)]
    largest = most if full else min(most, max(-(-total // number_of), total * weights[0] // sum(weights)))
    least = 1 if total - largest >= number_of - 1 else 0
    counts, rest = [largest] + [least] * (number_of - 1), total - largest - least * (number_of - 1)
    while rest > 0:
        candidates = [i for i in range(1, number_of) if counts[i] < largest] or [i for i in range(1, number_of) if counts[i] < most]
        pool, remaining = sum([weights[i] for i in candidates]), rest
        for i in candidates:
            extra = min(most - counts[i], max(1, remaining * weights[i] // pool), rest)
            counts[i] = counts[i] + extra
            rest = rest - extra
    return np.array(counts)


def centred(key, dims, scale, most, split=(), held_as=jnp.bfloat16):
    level = shard_levels(key, dims, split, -0.22, 0.18) if split else 1.0
    values = jax.random.normal(key, dims, jnp.float32) * scale * level
    return jnp.minimum(jnp.maximum(values, -most), most).astype(held_as)


def setup_inputs(seed: int = 0) -> dict:
    seeds = jax.random.split(jax.random.key(seed), 4)
    noise = centred(seeds[0], (FIELDS, 2, L, L), 1.0, 6.0, ((0, 32),))
    root = jnp.clip(jnp.exp(math.log(2.0) - 2.0794415 * jax.random.uniform(seeds[1], (FIELDS, L, L), jnp.float32) ** shard_levels(seeds[1], (FIELDS, L, L), ((0, 32),), -0.2, 0.2)), 0.25, 2.0).astype(jnp.bfloat16)
    home_keys = jax.random.split(jax.random.fold_in(seeds[2], 1), FIELDS // FSRC)
    home_turns = jax.random.permutation(jax.random.fold_in(seeds[2], 3), FIELDS // FSRC)
    home = jax.vmap(lambda own, number: shared_out(jax.random.fold_in(seeds[2], 2), own, number, FSRC, N_GRP, 1, CAP, 1))(home_keys, home_turns).reshape((FIELDS, 1))
    return dict(noise=noise, root=root, home=home)


def tables(length):
    index = jnp.arange(length, dtype=jnp.int32)
    product = (index[:, None] * index[None, :]) % length
    angle = product.astype(jnp.float32) * (2.0 * math.pi / length)
    return jnp.cos(angle).astype(jnp.bfloat16), jnp.sin(angle).astype(jnp.bfloat16)


def slots_of(homes):
    count = homes.shape[0]
    order = jnp.arange(count, dtype=jnp.int32)
    earlier = (homes[None, :] == homes[:, None]) & (order[None, :] < order[:, None])
    return jnp.sum(earlier.astype(jnp.int32), axis=1).astype(jnp.int32)


def reference(noise, root, home):
    cosine, sine_table = tables(L)
    cos_wide = cosine.astype(jnp.float32)
    sin_wide = sine_table.astype(jnp.float32)
    high = lax.Precision.HIGHEST

    def one_source(block):
        noise_block, root_block = block
        scale = root_block.astype(jnp.float32)
        spec_real = (noise_block[:, 0].astype(jnp.float32) * scale).astype(jnp.bfloat16).astype(jnp.float32)
        spec_imag = (noise_block[:, 1].astype(jnp.float32) * scale).astype(jnp.bfloat16).astype(jnp.float32)
        a_real = (jnp.einsum('frm,mn->frn', spec_real, cos_wide, precision=high)
                  + jnp.einsum('frm,mn->frn', spec_imag, sin_wide, precision=high)).astype(jnp.bfloat16)
        a_imag = (jnp.einsum('frm,mn->frn', spec_imag, cos_wide, precision=high)
                  - jnp.einsum('frm,mn->frn', spec_real, sin_wide, precision=high)).astype(jnp.bfloat16)
        turned = (jnp.einsum('frb,ra->fba', a_real.astype(jnp.float32), cos_wide, precision=high)
                  + jnp.einsum('frb,ra->fba', a_imag.astype(jnp.float32), sin_wide, precision=high))
        return (turned * (1.0 / L)).astype(jnp.bfloat16)

    fields = lax.map(one_source, (noise.reshape(N_GRP, FSRC, 2, L, L), root.reshape(N_GRP, FSRC, L, L)))
    homes = home[:, 0].astype(jnp.int32)
    slots = jax.vmap(slots_of)(homes.reshape(N_GRP, FSRC)).reshape(-1)
    source = (jnp.arange(N_GRP * FSRC, dtype=jnp.int32) // FSRC).astype(jnp.int32)
    sample = jnp.zeros((N_GRP, N_GRP, CAP, L, L), jnp.bfloat16)
    return sample.at[homes, source, slots].set(fields.reshape(N_GRP * FSRC, L, L))
```

```python
import functools
import math

import jax
import jax.numpy as jnp
import numpy as np
from jax import lax
from jax.experimental import pallas as pl
from jax.experimental.pallas import tpu as pltpu
from jax.sharding import PartitionSpec as P

CAP = 2


def tables(length):
    index = np.arange(length, dtype=np.int32)
    product = index[:, None] * index[None, :] % length
    angle = product.astype(np.float32) * np.float32(2.0 * math.pi / length)
    return (jnp.asarray(np.cos(angle), jnp.bfloat16), jnp.asarray(np.sin(angle), jnp.bfloat16))


def slots_of(homes):
    order = jnp.arange(homes.shape[0], dtype=jnp.int32)
    earlier = (homes[None, :] == homes[:, None]) & (order[None, :] < order[:, None])
    return jnp.sum(earlier.astype(jnp.int32), axis=1)


def field_body(fields, noise_ref, root_ref, first_ref, second_ref, outs, spec_ref):
    step = pl.program_id(0)
    length = root_ref.shape[-1]
    occupied = fields[step] >= 0

    def store(value):
        for j, out in enumerate(outs):

            @pl.when(step // CAP == j)
            def _():
                out[0] = value

    @pl.when(occupied)
    def _():
        scale = root_ref[0]
        spec_ref[:, :length] = noise_ref[0, 0] * scale
        spec_ref[:, length:] = noise_ref[0, 1] * scale
        turned = lax.dot_general(
            first_ref[...], spec_ref[...], (((1,), (1,)), ((), ())), preferred_element_type=jnp.float32
        ).astype(jnp.bfloat16)
        total = jnp.dot(turned[:length], second_ref[0], preferred_element_type=jnp.float32)
        total = total + jnp.dot(turned[length:], second_ref[1], preferred_element_type=jnp.float32)
        store((total * (1.0 / length)).astype(jnp.bfloat16))

    @pl.when(jnp.logical_not(occupied))
    def _():
        store(jnp.zeros((length, length), jnp.bfloat16))


def chunk_kernel(fields, noise_ref, root_ref, first_ref, second_ref, *rest):
    *outs, spec_ref = rest
    field_body(fields, noise_ref, root_ref, first_ref, second_ref, outs, spec_ref)


def own_kernel(fields, place, noise_ref, root_ref, first_ref, second_ref, out, spec_ref):
    field_body(fields, noise_ref, root_ref, first_ref, second_ref, [out.at[0]], spec_ref)


def picked(step, fields, *_):
    return (jnp.maximum(fields[step], 0), 0, 0)


def picked_pair(step, fields, *_):
    return (jnp.maximum(fields[step], 0), 0, 0, 0)


def in_specs_of(length):
    return [
        pl.BlockSpec((1, 2, length, length), picked_pair),
        pl.BlockSpec((1, length, length), picked),
        pl.BlockSpec((2 * length, 2 * length), lambda *_: (0, 0)),
        pl.BlockSpec((2, length, length), lambda *_: (0, 0, 0)),
    ]


def estimate(length, fields):
    return pl.CostEstimate(
        flops=12 * length**3 * fields, bytes_accessed=8 * length**2 * fields, transcendentals=0
    )


def out_place(j, step, *_):
    return (jnp.clip(step - CAP * j, 0, CAP - 1), 0, 0)


def chunk(fields, noise, root, first, second, dests):
    length = root.shape[-1]
    steps = dests * CAP
    return pl.pallas_call(
        chunk_kernel,
        grid_spec=pltpu.PrefetchScalarGridSpec(
            num_scalar_prefetch=1,
            grid=(steps,),
            in_specs=in_specs_of(length),
            out_specs=[
                pl.BlockSpec((1, length, length), functools.partial(out_place, j)) for j in range(dests)
            ],
            scratch_shapes=[pltpu.VMEM((length, 2 * length), jnp.bfloat16)],
        ),
        out_shape=[jax.ShapeDtypeStruct((CAP, length, length), jnp.bfloat16)] * dests,
        cost_estimate=estimate(length, steps),
        name=f"fields{dests}",
    )(fields, noise, root, first, second)


def own(fields, me, noise, root, first, second, groups):
    length = root.shape[-1]
    return pl.pallas_call(
        own_kernel,
        grid_spec=pltpu.PrefetchScalarGridSpec(
            num_scalar_prefetch=2,
            grid=(CAP,),
            in_specs=in_specs_of(length),
            out_specs=pl.BlockSpec(
                (1, 1, length, length), lambda step, fields, place: (place[0], step, 0, 0)
            ),
            scratch_shapes=[pltpu.VMEM((length, 2 * length), jnp.bfloat16)],
        ),
        out_shape=jax.ShapeDtypeStruct((groups, CAP, length, length), jnp.bfloat16),
        cost_estimate=estimate(length, CAP),
        name="fields_own",
    )(fields, me, noise, root, first, second)


def to_of(me, k, groups):
    return me ^ k if groups & (groups - 1) == 0 else (me + k) % groups


def from_of(me, k, groups):
    return me ^ k if groups & (groups - 1) == 0 else (me - k) % groups


def order_of(groups):
    far = [k for k in range(groups) if k >= groups // 2]
    near = [k for k in range(1, groups) if k < groups // 2]
    order = []
    while far or near:
        if far:
            order.append(far.pop(0))
        if near:
            order.append(near.pop(0))
    return order


def chunks_of(count):
    sizes, size, left = [], 1, count
    while left:
        size = min(size, left)
        sizes.append(size)
        left -= size
        size = min(2 * size, 4)
    return sizes


def local(noise, root, home):
    groups = lax.axis_size("grp")
    count, _, length = root.shape
    cosine, sine_table = tables(length)
    first = jnp.concatenate(
        [
            jnp.concatenate([cosine, sine_table], axis=1),
            jnp.concatenate([-sine_table, cosine], axis=1),
        ],
        axis=0,
    )
    second = jnp.stack([cosine, sine_table])
    me = lax.axis_index("grp")
    homes = lax.dynamic_slice_in_dim(home[:, 0], me * count, count)
    target = homes * CAP + slots_of(homes)
    order = order_of(groups)
    ks = jnp.asarray(order + [0], jnp.int32)
    partner = to_of(me, ks, groups)
    places = (partner[:, None] * CAP + jnp.arange(CAP, dtype=jnp.int32)[None, :]).reshape(-1)
    hit = places[:, None] == target[None, :]
    fields = jnp.max(jnp.where(hit, jnp.arange(count, dtype=jnp.int32)[None, :], -1), axis=1)
    received = []
    at = 0
    for dests in chunks_of(groups - 1):
        outs = chunk(fields[at * CAP : (at + dests) * CAP], noise, root, first, second, dests)
        for j in range(dests):
            k = order[at + j]
            pairs = [(i, to_of(i, k, groups)) for i in range(groups)]
            received.append((k, lax.ppermute(outs[j], "grp", pairs)))
        at += dests
    sample = own(fields[at * CAP :], me.reshape(1), noise, root, first, second, groups)
    for k, block in received:
        sample = lax.dynamic_update_slice_in_dim(sample, block[None], from_of(me, k, groups), 0)
    return sample[None]


def route_matrix(homes, groups):
    count = homes.shape[0]
    order = jnp.arange(count, dtype=jnp.int32)
    earlier = (homes[None, :] == homes[:, None]) & (order[None, :] < order[:, None])
    slots = jnp.sum(earlier.astype(jnp.int32), axis=1)
    target = homes * CAP + slots
    places = jnp.arange(groups * CAP, dtype=jnp.int32)
    return (places[:, None] == target[None, :]).astype(jnp.bfloat16)


def row_pass(spectra, cosine, sine_table, blocks):
    real_part = spectra[:, 0]
    imag_part = spectra[:, 1]
    length = cosine.shape[0]
    cos_split = cosine.reshape(length, blocks, length // blocks)
    sin_split = sine_table.reshape(length, blocks, length // blocks)
    a_real = (
        jnp.einsum("mjc,krm->jkrc", cos_split, real_part, preferred_element_type=jnp.float32)
        + jnp.einsum("mjc,krm->jkrc", sin_split, imag_part, preferred_element_type=jnp.float32)
    ).astype(jnp.bfloat16)
    a_imag = (
        jnp.einsum("mjc,krm->jkrc", cos_split, imag_part, preferred_element_type=jnp.float32)
        - jnp.einsum("mjc,krm->jkrc", sin_split, real_part, preferred_element_type=jnp.float32)
    ).astype(jnp.bfloat16)
    return (a_real, a_imag)


def column_pass(received, cosine, sine_table):
    a_real, a_imag = received
    senders, count, rows, cols = a_real.shape
    length = cosine.shape[0]
    cos_rows = cosine.reshape(senders, rows, length)
    sin_rows = sine_table.reshape(senders, rows, length)
    turned = jnp.einsum(
        "skrc,sra->kca", a_real, cos_rows, preferred_element_type=jnp.float32
    ) + jnp.einsum("skrc,sra->kca", a_imag, sin_rows, preferred_element_type=jnp.float32)
    return (turned * (1.0 / length)).astype(jnp.bfloat16)


def local_split(noise, root, home):
    groups = lax.axis_size("grp")
    blocks = lax.axis_size("fft")
    count, rows, length = root.shape
    cosine, sine_table = tables(length)
    source = lax.axis_index("grp")
    homes = lax.dynamic_slice_in_dim(home[:, 0], source * count, count)
    selector = route_matrix(homes, groups)
    scale = root[:, None].astype(jnp.float32)
    spectra = (noise.astype(jnp.float32) * scale).astype(jnp.bfloat16)
    a_real, a_imag = row_pass(spectra, cosine, sine_table, blocks)
    turned = column_pass(
        (
            lax.all_to_all(a_real, "fft", split_axis=0, concat_axis=0, tiled=True),
            lax.all_to_all(a_imag, "fft", split_axis=0, concat_axis=0, tiled=True),
        ),
        cosine,
        sine_table,
    )
    cols = turned.shape[1]
    outgoing = jnp.dot(
        selector, turned.reshape(count, cols * length), preferred_element_type=jnp.float32
    )
    outgoing = outgoing.astype(jnp.bfloat16).reshape(groups, CAP, cols, length)
    arrived = lax.all_to_all(outgoing, "grp", split_axis=0, concat_axis=0, tiled=True)
    return arrived[None]


def solution(mesh):
    return jax.shard_map(
        local if mesh.shape["fft"] == 1 else local_split,
        mesh=mesh,
        in_specs=(P("grp", None, "fft", None), P("grp", "fft", None), P()),
        out_specs=P("grp", None, None, "fft", None),
        check_vma=False,
    )
```

```python
import functools
import math

import jax
import jax.numpy as jnp
import numpy as np
from jax import lax
from jax.experimental import pallas as pl
from jax.experimental.pallas import tpu as pltpu
from jax.sharding import PartitionSpec as P

CAP = 2


def tables(length):
    index = np.arange(length, dtype=np.int32)
    product = index[:, None] * index[None, :] % length
    angle = product.astype(np.float32) * np.float32(2.0 * math.pi / length)
    return (jnp.asarray(np.cos(angle), jnp.bfloat16), jnp.asarray(np.sin(angle), jnp.bfloat16))


def turned_field(noise, root, cosine, sine_table):
    length = root.shape[-1]
    real_part, imag_part = noise[0] * root, noise[1] * root

    def over_second(table, part):
        return lax.dot_general(table, part, (((1,), (1,)), ((), ())), preferred_element_type=jnp.float32)

    a_real = over_second(cosine, real_part) + over_second(sine_table, imag_part)
    a_imag = over_second(cosine, imag_part) - over_second(sine_table, real_part)
    total = jnp.dot(a_real.astype(jnp.bfloat16), cosine, preferred_element_type=jnp.float32)
    total = total + jnp.dot(a_imag.astype(jnp.bfloat16), sine_table, preferred_element_type=jnp.float32)
    return (total * (1.0 / length)).astype(jnp.bfloat16)


def lead_kernel(
    groups, first_k, me_ref, position, home, noise, root, tables_hbm, fields, out,
    taken, noise_in, root_in, tables_in, arrived,
):
    count = noise.shape[0]
    me = me_ref[0]
    copies = [pltpu.make_async_copy(tables_hbm, tables_in, arrived.at[0])]
    copies[0].start()
    base = me * count
    goal = to_of(me, first_k, groups)
    chosen = jnp.int32(-1)
    for f in reversed(range(count)):
        chosen = jnp.where(home[0, base + f] == goal, f, chosen)
    source = jnp.maximum(chosen, 0)
    copies.append(pltpu.make_async_copy(noise.at[source], noise_in, arrived.at[1]))
    copies.append(pltpu.make_async_copy(root.at[source], root_in, arrived.at[2]))
    copies[1].start()
    copies[2].start()

    @pl.loop(0, groups)
    def _(g):
        taken[g] = 0

    @pl.loop(0, groups * CAP)
    def _(g):
        fields[g] = -1

    @pl.loop(0, count)
    def _(f):
        at = position[offset_of(me, home[0, base + f], groups)]
        slot = taken[at]
        fields[at * CAP + slot] = f
        taken[at] = slot + 1

    for copy in copies:
        copy.wait()

    @pl.when(chosen >= 0)
    def _():
        out[0] = turned_field(noise_in, root_in[...], tables_in[0], tables_in[1])

    @pl.when(chosen < 0)
    def _():
        out[...] = jnp.zeros_like(out)


def lead(me, position, home, noise, root, both, first_k):
    groups, length = position.shape[0], root.shape[-1]
    scalar = pl.BlockSpec(memory_space=pltpu.SMEM)
    whole = pl.BlockSpec(memory_space=pl.ANY)
    return pl.pallas_call(
        functools.partial(lead_kernel, groups, first_k),
        in_specs=[scalar, scalar, scalar, whole, whole, whole],
        out_specs=[scalar, pl.BlockSpec(memory_space=pltpu.VMEM)],
        out_shape=[
            jax.ShapeDtypeStruct((groups * CAP,), jnp.int32),
            jax.ShapeDtypeStruct((1, length, length), jnp.bfloat16),
        ],
        scratch_shapes=[
            pltpu.SMEM((groups,), jnp.int32),
            pltpu.VMEM((2, length, length), jnp.bfloat16),
            pltpu.VMEM((length, length), jnp.bfloat16),
            pltpu.VMEM((2, length, length), jnp.bfloat16),
            pltpu.SemaphoreType.DMA((3,)),
        ],
        cost_estimate=estimate(length, 1),
        name="fields_lead",
    )(me, position, home, noise, root, both)


def chunk_kernel(at, sizes, fields, me, noise, root, both, *outs):
    step = pl.program_id(0)
    occupied = fields[at + step] >= 0
    starts = np.cumsum([0] + sizes)

    def store(value):
        for j, out in enumerate(outs):

            @pl.when((step >= starts[j]) & (step < starts[j + 1]))
            def _():
                out[...] = value.reshape(out.shape)

    @pl.when(occupied)
    def _():
        store(turned_field(noise[0], root[0], both[0], both[1]))

    @pl.when(jnp.logical_not(occupied))
    def _():
        store(jnp.zeros(root.shape[1:], jnp.bfloat16))


def chunk(fields, me, noise, root, both, at, sizes, groups=None):
    length = root.shape[-1]
    steps = sum(sizes)
    starts = np.cumsum([0] + sizes)

    def picked(dims):
        return lambda step, fields, me: (jnp.maximum(fields[at + step], 0),) + (0,) * dims

    def placed(j):
        return lambda step, fields, me: (jnp.clip(step - starts[j], 0, sizes[j] - 1), 0, 0)

    if groups:
        out_specs = [pl.BlockSpec((1, 1, length, length), lambda step, fields, me: (me[0], step, 0, 0))]
        out_shape = [jax.ShapeDtypeStruct((groups, CAP, length, length), jnp.bfloat16)]
    else:
        out_specs = [pl.BlockSpec((1, length, length), placed(j)) for j in range(len(sizes))]
        out_shape = [jax.ShapeDtypeStruct((size, length, length), jnp.bfloat16) for size in sizes]
    return pl.pallas_call(
        functools.partial(chunk_kernel, at, sizes),
        grid_spec=pltpu.PrefetchScalarGridSpec(
            num_scalar_prefetch=2,
            grid=(steps,),
            in_specs=[
                pl.BlockSpec((1, 2, length, length), picked(3)),
                pl.BlockSpec((1, length, length), picked(2)),
                pl.BlockSpec((2, length, length), lambda *_: (0, 0, 0)),
            ],
            out_specs=out_specs,
        ),
        out_shape=out_shape,
        cost_estimate=estimate(length, steps),
        name=f"fields_from_{at}",
    )(fields, me, noise, root, both)


def estimate(length, fields):
    return pl.CostEstimate(
        flops=12 * length**3 * fields, bytes_accessed=8 * length**2 * fields, transcendentals=0
    )


def to_of(me, k, groups):
    return me ^ k if groups & (groups - 1) == 0 else (me + k) % groups


def from_of(me, k, groups):
    return me ^ k if groups & (groups - 1) == 0 else (me - k) % groups


def offset_of(me, other, groups):
    return me ^ other if groups & (groups - 1) == 0 else lax.rem(other - me + groups, groups)


def order_of(groups):
    far, near = list(range(groups // 2, groups)), list(range(groups // 2 - 1, 0, -1))
    order = far[:1]
    for pair in zip(far[1:], near):
        order.extend(pair)
    return order + far[1 + len(near) :] + near[len(far) - 1 :]


def local(noise, root, home):
    groups = lax.axis_size("grp")
    length = root.shape[-1]
    both = jnp.stack(tables(length))
    mine = lax.axis_index("grp")
    me = mine.astype(jnp.int32).reshape(1)
    order = order_of(groups) + [0]
    position = np.zeros((groups,), np.int32)
    position[order] = np.arange(groups)
    fields, block = lead(me, jnp.asarray(position), home.T, noise, root, both, order[0])
    received = []

    def send(block, j, slot):
        pairs = [(i, to_of(i, order[j], groups)) for i in range(groups)]
        received.append((order[j], slot, lax.ppermute(block, "grp", pairs)))

    send(block, 0, 0)
    send(chunk(fields, me, noise, root, both, 1, [CAP - 1])[0], 0, 1)
    j, width = 1, 1
    while j < groups - 1:
        width = min(width, groups - 1 - j)
        blocks = chunk(fields, me, noise, root, both, j * CAP, [CAP] * width)
        for i, block in enumerate(blocks):
            send(block, j + i, 0)
        j += width
        width = min(2 * width, 4)
    (sample,) = chunk(fields, me, noise, root, both, j * CAP, [CAP], groups)
    for k, slot, block in received:
        sample = lax.dynamic_update_slice(sample, block[None], (from_of(mine, k, groups), slot, 0, 0))
    return sample[None]


def route_matrix(homes, groups):
    count = homes.shape[0]
    order = jnp.arange(count, dtype=jnp.int32)
    earlier = (homes[None, :] == homes[:, None]) & (order[None, :] < order[:, None])
    slots = jnp.sum(earlier.astype(jnp.int32), axis=1)
    target = homes * CAP + slots
    places = jnp.arange(groups * CAP, dtype=jnp.int32)
    return (places[:, None] == target[None, :]).astype(jnp.bfloat16)


def row_pass(spectra, cosine, sine_table, blocks):
    real_part = spectra[:, 0]
    imag_part = spectra[:, 1]
    length = cosine.shape[0]
    cos_split = cosine.reshape(length, blocks, length // blocks)
    sin_split = sine_table.reshape(length, blocks, length // blocks)
    a_real = (
        jnp.einsum("mjc,krm->jkrc", cos_split, real_part, preferred_element_type=jnp.float32)
        + jnp.einsum("mjc,krm->jkrc", sin_split, imag_part, preferred_element_type=jnp.float32)
    ).astype(jnp.bfloat16)
    a_imag = (
        jnp.einsum("mjc,krm->jkrc", cos_split, imag_part, preferred_element_type=jnp.float32)
        - jnp.einsum("mjc,krm->jkrc", sin_split, real_part, preferred_element_type=jnp.float32)
    ).astype(jnp.bfloat16)
    return (a_real, a_imag)


def column_pass(received, cosine, sine_table):
    a_real, a_imag = received
    senders, count, rows, cols = a_real.shape
    length = cosine.shape[0]
    cos_rows = cosine.reshape(senders, rows, length)
    sin_rows = sine_table.reshape(senders, rows, length)
    turned = jnp.einsum(
        "skrc,sra->kca", a_real, cos_rows, preferred_element_type=jnp.float32
    ) + jnp.einsum("skrc,sra->kca", a_imag, sin_rows, preferred_element_type=jnp.float32)
    return (turned * (1.0 / length)).astype(jnp.bfloat16)


def local_split(noise, root, home):
    groups = lax.axis_size("grp")
    blocks = lax.axis_size("fft")
    count, rows, length = root.shape
    cosine, sine_table = tables(length)
    source = lax.axis_index("grp")
    homes = lax.dynamic_slice_in_dim(home[:, 0], source * count, count)
    selector = route_matrix(homes, groups)
    scale = root[:, None].astype(jnp.float32)
    spectra = (noise.astype(jnp.float32) * scale).astype(jnp.bfloat16)
    a_real, a_imag = row_pass(spectra, cosine, sine_table, blocks)
    turned = column_pass(
        (
            lax.all_to_all(a_real, "fft", split_axis=0, concat_axis=0, tiled=True),
            lax.all_to_all(a_imag, "fft", split_axis=0, concat_axis=0, tiled=True),
        ),
        cosine,
        sine_table,
    )
    cols = turned.shape[1]
    outgoing = jnp.dot(
        selector, turned.reshape(count, cols * length), preferred_element_type=jnp.float32
    )
    outgoing = outgoing.astype(jnp.bfloat16).reshape(groups, CAP, cols, length)
    arrived = lax.all_to_all(outgoing, "grp", split_axis=0, concat_axis=0, tiled=True)
    return arrived[None]


def solution(mesh):
    return jax.shard_map(
        local if mesh.shape["fft"] == 1 else local_split,
        mesh=mesh,
        in_specs=(P("grp", None, "fft", None), P("grp", "fft", None), P()),
        out_specs=P("grp", None, None, "fft", None),
        check_vma=False,
    )
```

```python
import functools
import math

import jax
import jax.numpy as jnp
import numpy as np
from jax import lax
from jax.experimental import pallas as pl
from jax.experimental.pallas import tpu as pltpu
from jax.sharding import PartitionSpec as P

CAP = 2


def tables(length):
    index = np.arange(length, dtype=np.int32)
    product = index[:, None] * index[None, :] % length
    angle = product.astype(np.float32) * np.float32(2.0 * math.pi / length)
    return (jnp.asarray(np.cos(angle), jnp.bfloat16), jnp.asarray(np.sin(angle), jnp.bfloat16))


def turned_field(noise, root, cosine, sine_table):
    length = root.shape[-1]
    real_part, imag_part = noise[0] * root, noise[1] * root

    def over_second(table, part):
        return lax.dot_general(table, part, (((1,), (1,)), ((), ())), preferred_element_type=jnp.float32)

    a_real = over_second(cosine, real_part) + over_second(sine_table, imag_part)
    a_imag = over_second(cosine, imag_part) - over_second(sine_table, real_part)
    total = jnp.dot(a_real.astype(jnp.bfloat16), cosine, preferred_element_type=jnp.float32)
    total = total + jnp.dot(a_imag.astype(jnp.bfloat16), sine_table, preferred_element_type=jnp.float32)
    return (total * (1.0 / length)).astype(jnp.bfloat16)


def lead_kernel(
    groups, first_k, me_ref, home, noise, root, tables_hbm, fields, out,
    taken, noise_in, root_in, tables_in, arrived,
):
    count = noise.shape[0]
    me = me_ref[0]
    copies = [pltpu.make_async_copy(tables_hbm, tables_in, arrived.at[0])]
    copies[0].start()
    base = me * count
    goal = to_of(me, first_k, groups)
    chosen = jnp.int32(-1)
    for f in reversed(range(count)):
        chosen = jnp.where(home[0, base + f] == goal, f, chosen)
    source = jnp.maximum(chosen, 0)
    copies.append(pltpu.make_async_copy(noise.at[source], noise_in, arrived.at[1]))
    copies.append(pltpu.make_async_copy(root.at[source], root_in, arrived.at[2]))
    copies[1].start()
    copies[2].start()

    for g in range(groups):
        taken[g] = 0
    for g in range(groups * CAP):
        fields[g] = -1

    @pl.loop(0, count, unroll=4)
    def _(f):
        at = place_of(offset_of(me, home[0, base + f], groups), groups)
        slot = taken[at]
        fields[at * CAP + slot] = f
        taken[at] = slot + 1

    for copy in copies:
        copy.wait()

    @pl.when(chosen >= 0)
    def _():
        out[0] = turned_field(noise_in, root_in[...], tables_in[0], tables_in[1])

    @pl.when(chosen < 0)
    def _():
        out[...] = jnp.zeros_like(out)


def lead(me, home, noise, root, both, first_k, groups):
    length = root.shape[-1]
    scalar = pl.BlockSpec(memory_space=pltpu.SMEM)
    whole = pl.BlockSpec(memory_space=pl.ANY)
    return pl.pallas_call(
        functools.partial(lead_kernel, groups, first_k),
        in_specs=[scalar, scalar, whole, whole, whole],
        out_specs=[scalar, pl.BlockSpec(memory_space=pltpu.VMEM)],
        out_shape=[
            jax.ShapeDtypeStruct((groups * CAP,), jnp.int32),
            pltpu.VMEM((1, length, length), jnp.bfloat16),
        ],
        scratch_shapes=[
            pltpu.SMEM((groups,), jnp.int32),
            pltpu.VMEM((2, length, length), jnp.bfloat16),
            pltpu.VMEM((length, length), jnp.bfloat16),
            pltpu.VMEM((2, length, length), jnp.bfloat16),
            pltpu.SemaphoreType.DMA((3,)),
        ],
        cost_estimate=estimate(length, 1),
        name="fields_lead",
    )(me, home, noise, root, both)


def chunk_kernel(at, sizes, fields, me, noise, root, both, *outs):
    step = pl.program_id(0)
    occupied = fields[at + step] >= 0
    starts = np.cumsum([0] + sizes)

    def store(value):
        for j, out in enumerate(outs):

            @pl.when((step >= starts[j]) & (step < starts[j + 1]))
            def _():
                out[...] = value.reshape(out.shape)

    @pl.when(occupied)
    def _():
        store(turned_field(noise[0], root[0], both[0], both[1]))

    @pl.when(jnp.logical_not(occupied))
    def _():
        store(jnp.zeros(root.shape[1:], jnp.bfloat16))


def chunk(fields, me, noise, root, both, at, sizes, groups=None):
    length = root.shape[-1]
    steps = sum(sizes)
    starts = np.cumsum([0] + sizes)

    def picked(dims):
        def index(step, fields, me):
            return (jnp.maximum(fields[at + jnp.minimum(step, steps - 1)], 0),) + (0,) * dims

        return index

    def placed(j):
        return lambda step, fields, me: (jnp.clip(step - starts[j], 0, sizes[j] - 1), 0, 0)

    if groups:
        out_specs = [pl.BlockSpec((1, 1, length, length), lambda step, fields, me: (me[0], step, 0, 0))]
        out_shape = [jax.ShapeDtypeStruct((groups, CAP, length, length), jnp.bfloat16)]
    else:
        out_specs = [pl.BlockSpec((1, length, length), placed(j)) for j in range(len(sizes))]
        out_shape = [jax.ShapeDtypeStruct((size, length, length), jnp.bfloat16) for size in sizes]
    return pl.pallas_call(
        functools.partial(chunk_kernel, at, sizes),
        grid_spec=pltpu.PrefetchScalarGridSpec(
            num_scalar_prefetch=2,
            grid=(steps,),
            in_specs=[
                pl.BlockSpec((1, 2, length, length), picked(3)),
                pl.BlockSpec((1, length, length), picked(2)),
                pl.BlockSpec((2, length, length), lambda *_: (0, 0, 0)),
            ],
            out_specs=out_specs,
        ),
        out_shape=out_shape,
        cost_estimate=estimate(length, steps),
        name=f"fields_from_{at}",
    )(fields, me, noise, root, both)


def estimate(length, fields):
    return pl.CostEstimate(
        flops=12 * length**3 * fields, bytes_accessed=8 * length**2 * fields, transcendentals=0
    )


def to_of(me, k, groups):
    return me ^ k if groups & (groups - 1) == 0 else (me + k) % groups


def from_of(me, k, groups):
    return me ^ k if groups & (groups - 1) == 0 else (me - k) % groups


def offset_of(me, other, groups):
    return me ^ other if groups & (groups - 1) == 0 else lax.rem(other - me + groups, groups)


def place_of(k, groups, xp=jnp):
    half = groups // 2
    turn = half + half // 2
    far = xp.where(k >= turn, turn + groups - 1 - k, k) - half
    return xp.where(k >= half, xp.maximum(2 * far - 1, 0), xp.minimum(2 * (half - k), groups - 1))


def local(noise, root, home):
    groups = lax.axis_size("grp")
    length = root.shape[-1]
    both = jnp.stack(tables(length))
    mine = lax.axis_index("grp")
    me = mine.astype(jnp.int32).reshape(1)
    order = np.argsort(place_of(np.arange(groups), groups, np)).tolist()
    fields, block = lead(me, home.T, noise, root, both, order[0], groups)
    received = []

    def send(block, j, slot):
        pairs = [(i, to_of(i, order[j], groups)) for i in range(groups)]
        received.append((order[j], slot, lax.ppermute(block, "grp", pairs)))

    send(block, 0, 0)
    send(chunk(fields, me, noise, root, both, 1, [CAP - 1])[0], 0, 1)
    j, width = 1, 1
    while j < groups - 1:
        width = min(width, groups - 1 - j)
        blocks = chunk(fields, me, noise, root, both, j * CAP, [CAP] * width)
        for i, block in enumerate(blocks):
            send(block, j + i, 0)
        j += width
        width = min(2 * width, 4)
    (sample,) = chunk(fields, me, noise, root, both, j * CAP, [CAP], groups)
    for k, slot, block in sorted(received, key=lambda entry: entry[0] == order[groups - 3]):
        sample = lax.dynamic_update_slice(sample, block[None], (from_of(mine, k, groups), slot, 0, 0))
    return sample[None]


def route_matrix(homes, groups):
    count = homes.shape[0]
    order = jnp.arange(count, dtype=jnp.int32)
    earlier = (homes[None, :] == homes[:, None]) & (order[None, :] < order[:, None])
    slots = jnp.sum(earlier.astype(jnp.int32), axis=1)
    target = homes * CAP + slots
    places = jnp.arange(groups * CAP, dtype=jnp.int32)
    return (places[:, None] == target[None, :]).astype(jnp.bfloat16)


def row_pass(spectra, cosine, sine_table, blocks):
    real_part = spectra[:, 0]
    imag_part = spectra[:, 1]
    length = cosine.shape[0]
    cos_split = cosine.reshape(length, blocks, length // blocks)
    sin_split = sine_table.reshape(length, blocks, length // blocks)
    a_real = (
        jnp.einsum("mjc,krm->jkrc", cos_split, real_part, preferred_element_type=jnp.float32)
        + jnp.einsum("mjc,krm->jkrc", sin_split, imag_part, preferred_element_type=jnp.float32)
    ).astype(jnp.bfloat16)
    a_imag = (
        jnp.einsum("mjc,krm->jkrc", cos_split, imag_part, preferred_element_type=jnp.float32)
        - jnp.einsum("mjc,krm->jkrc", sin_split, real_part, preferred_element_type=jnp.float32)
    ).astype(jnp.bfloat16)
    return (a_real, a_imag)


def column_pass(received, cosine, sine_table):
    a_real, a_imag = received
    senders, count, rows, cols = a_real.shape
    length = cosine.shape[0]
    cos_rows = cosine.reshape(senders, rows, length)
    sin_rows = sine_table.reshape(senders, rows, length)
    turned = jnp.einsum(
        "skrc,sra->kca", a_real, cos_rows, preferred_element_type=jnp.float32
    ) + jnp.einsum("skrc,sra->kca", a_imag, sin_rows, preferred_element_type=jnp.float32)
    return (turned * (1.0 / length)).astype(jnp.bfloat16)


def local_split(noise, root, home):
    groups = lax.axis_size("grp")
    blocks = lax.axis_size("fft")
    count, rows, length = root.shape
    cosine, sine_table = tables(length)
    source = lax.axis_index("grp")
    homes = lax.dynamic_slice_in_dim(home[:, 0], source * count, count)
    selector = route_matrix(homes, groups)
    scale = root[:, None].astype(jnp.float32)
    spectra = (noise.astype(jnp.float32) * scale).astype(jnp.bfloat16)
    a_real, a_imag = row_pass(spectra, cosine, sine_table, blocks)
    turned = column_pass(
        (
            lax.all_to_all(a_real, "fft", split_axis=0, concat_axis=0, tiled=True),
            lax.all_to_all(a_imag, "fft", split_axis=0, concat_axis=0, tiled=True),
        ),
        cosine,
        sine_table,
    )
    cols = turned.shape[1]
    outgoing = jnp.dot(
        selector, turned.reshape(count, cols * length), preferred_element_type=jnp.float32
    )
    outgoing = outgoing.astype(jnp.bfloat16).reshape(groups, CAP, cols, length)
    arrived = lax.all_to_all(outgoing, "grp", split_axis=0, concat_axis=0, tiled=True)
    return arrived[None]


def solution(mesh):
    return jax.shard_map(
        local if mesh.shape["fft"] == 1 else local_split,
        mesh=mesh,
        in_specs=(P("grp", None, "fft", None), P("grp", "fft", None), P()),
        out_specs=P("grp", None, None, "fft", None),
        check_vma=False,
    )
```

```python
import functools
import math

import jax
import jax.numpy as jnp
import numpy as np
from jax import lax
from jax.experimental import pallas as pl
from jax.experimental.pallas import tpu as pltpu
from jax.sharding import PartitionSpec as P

CAP = 2


def tables(length):
    index = np.arange(length, dtype=np.int32)
    product = index[:, None] * index[None, :] % length
    angle = product.astype(np.float32) * np.float32(2.0 * math.pi / length)
    return (jnp.asarray(np.cos(angle), jnp.bfloat16), jnp.asarray(np.sin(angle), jnp.bfloat16))


def turned_field(noise, root, cosine, sine_table):
    length = root.shape[-1]
    real_part, imag_part = noise[0] * root, noise[1] * root

    def over_second(table, part):
        return lax.dot_general(table, part, (((1,), (1,)), ((), ())), preferred_element_type=jnp.float32)

    a_real = over_second(cosine, real_part) + over_second(sine_table, imag_part)
    a_imag = over_second(cosine, imag_part) - over_second(sine_table, real_part)
    total = jnp.dot(a_real.astype(jnp.bfloat16), cosine, preferred_element_type=jnp.float32)
    total = total + jnp.dot(a_imag.astype(jnp.bfloat16), sine_table, preferred_element_type=jnp.float32)
    return (total * (1.0 / length)).astype(jnp.bfloat16)


def lead_kernel(
    groups, first_k, me_ref, home, noise, root, tables_hbm, fields, out,
    taken, noise_in, root_in, tables_in, arrived,
):
    count = noise.shape[0]
    me = me_ref[0]
    copies = [pltpu.make_async_copy(tables_hbm, tables_in, arrived.at[0])]
    copies[0].start()
    base = me * count
    goal = to_of(me, first_k, groups)
    chosen = jnp.int32(-1)
    for f in reversed(range(count)):
        chosen = jnp.where(home[0, base + f] == goal, f, chosen)
    source = jnp.maximum(chosen, 0)
    copies.append(pltpu.make_async_copy(noise.at[source], noise_in, arrived.at[1]))
    copies.append(pltpu.make_async_copy(root.at[source], root_in, arrived.at[2]))
    copies[1].start()
    copies[2].start()

    for g in range(groups):
        taken[g] = 0
    for g in range(groups * CAP):
        fields[g] = -1

    @pl.loop(0, count, unroll=4)
    def _(f):
        at = place_of(offset_of(me, home[0, base + f], groups), groups)
        slot = taken[at]
        fields[at * CAP + slot] = f
        taken[at] = slot + 1

    for copy in copies:
        copy.wait()

    @pl.when(chosen >= 0)
    def _():
        out[0] = turned_field(noise_in, root_in[...], tables_in[0], tables_in[1])

    @pl.when(chosen < 0)
    def _():
        out[...] = jnp.zeros_like(out)


def lead(me, home, noise, root, both, first_k, groups):
    length = root.shape[-1]
    scalar = pl.BlockSpec(memory_space=pltpu.SMEM)
    whole = pl.BlockSpec(memory_space=pl.ANY)
    return pl.pallas_call(
        functools.partial(lead_kernel, groups, first_k),
        in_specs=[scalar, scalar, whole, whole, whole],
        out_specs=[scalar, pl.BlockSpec(memory_space=pltpu.VMEM)],
        out_shape=[
            jax.ShapeDtypeStruct((groups * CAP,), jnp.int32),
            pltpu.VMEM((1, length, length), jnp.bfloat16),
        ],
        scratch_shapes=[
            pltpu.SMEM((groups,), jnp.int32),
            pltpu.VMEM((2, length, length), jnp.bfloat16),
            pltpu.VMEM((length, length), jnp.bfloat16),
            pltpu.VMEM((2, length, length), jnp.bfloat16),
            pltpu.SemaphoreType.DMA((3,)),
        ],
        cost_estimate=estimate(length, 1),
        name="fields_lead",
    )(me, home, noise, root, both)


def chunk_kernel(at, sizes, fields, me, noise, root, both, *outs):
    step = pl.program_id(0)
    occupied = fields[at + step] >= 0
    starts = np.cumsum([0] + sizes)

    def store(value):
        for j, out in enumerate(outs):

            @pl.when((step >= starts[j]) & (step < starts[j + 1]))
            def _():
                out[...] = value.reshape(out.shape)

    @pl.when(occupied)
    def _():
        store(turned_field(noise[0], root[0], both[0], both[1]))

    @pl.when(jnp.logical_not(occupied))
    def _():
        store(jnp.zeros(root.shape[1:], jnp.bfloat16))


def chunk(fields, me, noise, root, both, at, sizes, groups=None):
    length = root.shape[-1]
    steps = sum(sizes)
    starts = np.cumsum([0] + sizes)

    def picked(dims):
        def index(step, fields, me):
            return (jnp.maximum(fields[at + jnp.minimum(step, steps - 1)], 0),) + (0,) * dims

        return index

    def placed(j):
        return lambda step, fields, me: (jnp.clip(step - starts[j], 0, sizes[j] - 1), 0, 0)

    if groups:
        out_specs = [pl.BlockSpec((1, 1, length, length), lambda step, fields, me: (me[0], step, 0, 0))]
        out_shape = [jax.ShapeDtypeStruct((groups, CAP, length, length), jnp.bfloat16)]
    else:
        out_specs = [pl.BlockSpec((1, length, length), placed(j)) for j in range(len(sizes))]
        out_shape = [jax.ShapeDtypeStruct((size, length, length), jnp.bfloat16) for size in sizes]
    return pl.pallas_call(
        functools.partial(chunk_kernel, at, sizes),
        grid_spec=pltpu.PrefetchScalarGridSpec(
            num_scalar_prefetch=2,
            grid=(steps,),
            in_specs=[
                pl.BlockSpec((1, 2, length, length), picked(3)),
                pl.BlockSpec((1, length, length), picked(2)),
                pl.BlockSpec((2, length, length), lambda *_: (0, 0, 0)),
            ],
            out_specs=out_specs,
        ),
        out_shape=out_shape,
        cost_estimate=estimate(length, steps),
        name=f"fields_from_{at}",
    )(fields, me, noise, root, both)


def estimate(length, fields):
    return pl.CostEstimate(
        flops=12 * length**3 * fields, bytes_accessed=8 * length**2 * fields, transcendentals=0
    )


def to_of(me, k, groups):
    return me ^ k if groups & (groups - 1) == 0 else (me + k) % groups


def from_of(me, k, groups):
    return me ^ k if groups & (groups - 1) == 0 else (me - k) % groups


def offset_of(me, other, groups):
    return me ^ other if groups & (groups - 1) == 0 else lax.rem(other - me + groups, groups)


def place_of(k, groups, xp=jnp):
    half = groups // 2
    turn = half + half // 2
    far = xp.where(k >= turn, turn + groups - 1 - k, k) - half
    return xp.where(k >= half, xp.maximum(2 * far - 1, 0), xp.minimum(2 * (half - k), groups - 1))


def local(noise, root, home):
    groups = lax.axis_size("grp")
    length = root.shape[-1]
    both = jnp.stack(tables(length))
    mine = lax.axis_index("grp")
    me = mine.astype(jnp.int32).reshape(1)
    order = np.argsort(place_of(np.arange(groups), groups, np)).tolist()
    fields, block = lead(me, home.T, noise, root, both, order[0], groups)
    received = []

    def send(block, j, slot):
        pairs = [(i, to_of(i, order[j], groups)) for i in range(groups)[:: -1 if slot else 1]]
        received.append((order[j], slot, lax.ppermute(block, "grp", pairs)))

    send(block, 0, 0)
    send(chunk(fields, me, noise, root, both, 1, [CAP - 1])[0], 0, 1)
    j, width = 1, 1
    while j < groups - 1:
        width = min(width, groups - 1 - j)
        blocks = chunk(fields, me, noise, root, both, j * CAP, [CAP] * width)
        for i, block in enumerate(blocks):
            send(block, j + i, 0)
        j += width
        width = min(2 * width, 4)
    (sample,) = chunk(fields, me, noise, root, both, j * CAP, [CAP], groups)
    for k, slot, block in sorted(received, key=lambda entry: entry[0] == order[groups - 3]):
        sample = lax.dynamic_update_slice(sample, block[None], (from_of(mine, k, groups), slot, 0, 0))
    return sample[None]


def route_matrix(homes, groups):
    count = homes.shape[0]
    order = jnp.arange(count, dtype=jnp.int32)
    earlier = (homes[None, :] == homes[:, None]) & (order[None, :] < order[:, None])
    slots = jnp.sum(earlier.astype(jnp.int32), axis=1)
    target = homes * CAP + slots
    places = jnp.arange(groups * CAP, dtype=jnp.int32)
    return (places[:, None] == target[None, :]).astype(jnp.bfloat16)


def row_pass(spectra, cosine, sine_table, blocks):
    real_part = spectra[:, 0]
    imag_part = spectra[:, 1]
    length = cosine.shape[0]
    cos_split = cosine.reshape(length, blocks, length // blocks)
    sin_split = sine_table.reshape(length, blocks, length // blocks)
    a_real = (
        jnp.einsum("mjc,krm->jkrc", cos_split, real_part, preferred_element_type=jnp.float32)
        + jnp.einsum("mjc,krm->jkrc", sin_split, imag_part, preferred_element_type=jnp.float32)
    ).astype(jnp.bfloat16)
    a_imag = (
        jnp.einsum("mjc,krm->jkrc", cos_split, imag_part, preferred_element_type=jnp.float32)
        - jnp.einsum("mjc,krm->jkrc", sin_split, real_part, preferred_element_type=jnp.float32)
    ).astype(jnp.bfloat16)
    return (a_real, a_imag)


def column_pass(received, cosine, sine_table):
    a_real, a_imag = received
    senders, count, rows, cols = a_real.shape
    length = cosine.shape[0]
    cos_rows = cosine.reshape(senders, rows, length)
    sin_rows = sine_table.reshape(senders, rows, length)
    turned = jnp.einsum(
        "skrc,sra->kca", a_real, cos_rows, preferred_element_type=jnp.float32
    ) + jnp.einsum("skrc,sra->kca", a_imag, sin_rows, preferred_element_type=jnp.float32)
    return (turned * (1.0 / length)).astype(jnp.bfloat16)


def local_split(noise, root, home):
    groups = lax.axis_size("grp")
    blocks = lax.axis_size("fft")
    count, rows, length = root.shape
    cosine, sine_table = tables(length)
    source = lax.axis_index("grp")
    homes = lax.dynamic_slice_in_dim(home[:, 0], source * count, count)
    selector = route_matrix(homes, groups)
    scale = root[:, None].astype(jnp.float32)
    spectra = (noise.astype(jnp.float32) * scale).astype(jnp.bfloat16)
    a_real, a_imag = row_pass(spectra, cosine, sine_table, blocks)
    turned = column_pass(
        (
            lax.all_to_all(a_real, "fft", split_axis=0, concat_axis=0, tiled=True),
            lax.all_to_all(a_imag, "fft", split_axis=0, concat_axis=0, tiled=True),
        ),
        cosine,
        sine_table,
    )
    cols = turned.shape[1]
    outgoing = jnp.dot(
        selector, turned.reshape(count, cols * length), preferred_element_type=jnp.float32
    )
    outgoing = outgoing.astype(jnp.bfloat16).reshape(groups, CAP, cols, length)
    arrived = lax.all_to_all(outgoing, "grp", split_axis=0, concat_axis=0, tiled=True)
    return arrived[None]


def solution(mesh):
    return jax.shard_map(
        local if mesh.shape["fft"] == 1 else local_split,
        mesh=mesh,
        in_specs=(P("grp", None, "fft", None), P("grp", "fft", None), P()),
        out_specs=P("grp", None, None, "fft", None),
        check_vma=False,
    )
```
